32 devices in a mesh: batch: 8 (over z, x), cols: 4 (over y, core).
Axes of the slice: x: 2, y: 2, z: 4, core: 2. Of those that a mesh axis runs over, the one named last changes fastest.
Arguments:
- partial_query: float32 [8, 1024, 1024], P('batch', None, 'cols'), may hold values from -0.875 to 0.875
- partial_key: float32 [8, 1024, 1024], P('batch', None, 'cols'), may hold values from -0.875 to 0.875
- partial_value: float32 [8, 1024, 1024], P('batch', None, 'cols'), may hold values from -0.875 to 0.875
- partial_mixed: float32 [8, 1024, 1024], P('batch', 'cols'), may hold values from -0.875 to 0.875
- partial_norm: float32 [8, 1024], P('batch'), may hold values from -8 to 8
- partial_bias: float32 [8, 1024], P('batch'), may hold values from -8 to 8
- master_query: float32 [1024, 1024], P('batch', 'cols'), may hold values from -0.1875 to 0.1875
- master_key: float32 [1024, 1024], P('batch', 'cols'), may hold values from -0.1875 to 0.1875
- master_value: float32 [1024, 1024], P('batch', 'cols'), may hold values from -0.1875 to 0.1875
- master_mixed: float32 [1024, 1024], P('cols', 'batch'), may hold values from -0.1875 to 0.1875
- master_norm: float32 [1024], P('batch'), may hold values from 0.25 to 1.75
- master_bias: float32 [1024], P('batch'), may hold values from -3 to 3
Outputs:
- compute_query: bfloat16 [1024, 1024], P(None, 'cols')
- compute_key: bfloat16 [1024, 1024], P(None, 'cols')
- compute_value: bfloat16 [1024, 1024], P(None, 'cols')
- compute_mixed: bfloat16 [1024, 1024], P('cols')
- compute_norm: bfloat16 [1024], replicated
- compute_bias: bfloat16 [1024], replicated
- stepped_query: float32 [1024, 1024], P('batch', 'cols')
- stepped_key: float32 [1024, 1024], P('batch', 'cols')
- stepped_value: float32 [1024, 1024], P('batch', 'cols')
- stepped_mixed: float32 [1024, 1024], P('cols', 'batch')
- stepped_norm: float32 [1024], P('batch')
- stepped_bias: float32 [1024], P('batch')
The draws below stay inside these ranges and needn't reach their ends.
All inputs are finite; a program needn't handle non-finite values.
Results may differ from the reference program's by a relative error of at most 0.001.
Values may be sent and summed in bfloat16 or wider, within the bound.
A program may use at most 64 MiB of HBM per device.

```python
import jax
import jax.numpy as jnp

WIDTH = 1024
ATTN = 1024
REPLICAS = 8


def with_spikes(array, stream_key, source, target, blocks, factor):
    owner, partner = [(jnp.arange(array.shape[axis_at]) // (array.shape[axis_at] // blocks)).reshape([-1 if axis == axis_at else 1 for axis in range(array.ndim)]) for axis_at in (source, target)]
    chosen = jax.random.permutation(stream_key, blocks)[partner]
    strong = (owner == chosen) | (owner == (partner + blocks // 2) % blocks)
    return jnp.where(strong, factor * array, array)


def levels(rng, extent, cuts, smallest, top_value):
    def one(position, blocks):
        heights = jax.random.uniform(jax.random.fold_in(jax.random.fold_in(rng, 6), position), (blocks,), jnp.float32, smallest / len(cuts), top_value / len(cuts))
        return jnp.repeat(jnp.exp(heights), extent[position] // blocks).reshape((-1,) + (1,) * (len(extent) - position - 1))

    loudness = one(*cuts[0])
    for cut in cuts[1:]:
        loudness = loudness * one(*cut)
    return loudness


def gaussian(stream_key, extent, spread, limit, shards=(), dtype=jnp.bfloat16):
    loudness = levels(stream_key, extent, shards, -0.22, 0.18) if shards else 1.0
    drawn = jax.random.normal(stream_key, extent, jnp.float32) * spread * loudness
    return jnp.minimum(jnp.maximum(drawn, -limit), limit).astype(dtype)


def heavy_noise(stream_key, dims, deviation, reach, cuts, heavy, kind=jnp.bfloat16):
    drawn = deviation * jax.random.normal(stream_key, dims, jnp.float32)
    if cuts:
        drawn = drawn * levels(stream_key, dims, cuts, -0.22, 0.18)
    return jnp.clip(with_spikes(drawn, jax.random.fold_in(stream_key, 3), *heavy), -reach, reach).astype(kind)


def setup_inputs(seed: int = 0) -> dict:
    splits = jax.random.split(jax.random.key(seed), 13)
    partial_query = heavy_noise(splits[0], (REPLICAS, WIDTH, ATTN), 0.1, 0.875, ((0, 8), (2, 4)), (0, 1, 8, 2.0), jnp.float32)
    partial_key = heavy_noise(splits[1], (REPLICAS, WIDTH, ATTN), 0.1, 0.875, ((0, 8), (2, 4)), (0, 1, 8, 2.0), jnp.float32)
    partial_value = heavy_noise(splits[2], (REPLICAS, WIDTH, ATTN), 0.1, 0.875, ((0, 8), (2, 4)), (0, 1, 8, 2.0), jnp.float32)
    partial_mixed = heavy_noise(splits[3], (REPLICAS, ATTN, WIDTH), 0.1, 0.875, ((0, 8), (1, 4)), (0, 2, 8, 2.0), jnp.float32)
    partial_norm = heavy_noise(splits[4], (REPLICAS, WIDTH), 1.0, 8.0, ((0, 8),), (0, 1, 8, 2.0), jnp.float32)
    partial_bias = heavy_noise(splits[5], (REPLICAS, WIDTH), 1.0, 8.0, ((0, 8),), (0, 1, 8, 2.0), jnp.float32)
    master_query = gaussian(splits[6], (WIDTH, ATTN), WIDTH ** -0.5, 0.1875, ((0, 8), (1, 4)), jnp.float32)
    master_key = gaussian(splits[7], (WIDTH, ATTN), WIDTH ** -0.5, 0.1875, ((0, 8), (1, 4)), jnp.float32)
    master_value = gaussian(splits[8], (WIDTH, ATTN), WIDTH ** -0.5, 0.1875, ((0, 8), (1, 4)), jnp.float32)
    master_mixed = gaussian(splits[9], (ATTN, WIDTH), ATTN ** -0.5, 0.1875, ((0, 4), (1, 8)), jnp.float32)
    master_norm = jnp.clip(1.0 + 0.15 * jax.random.normal(splits[10], (WIDTH,), jnp.float32), 0.25, 1.75)
    master_bias = gaussian(splits[11], (WIDTH,), 0.5, 3.0, ((0, 8),), jnp.float32)
    return {"partial_query": partial_query, "partial_key": partial_key, "partial_value": partial_value, "partial_mixed": partial_mixed, "partial_norm": partial_norm, "partial_bias": partial_bias, "master_query": master_query, "master_key": master_key, "master_value": master_value, "master_mixed": master_mixed, "master_norm": master_norm, "master_bias": master_bias}


learn_rate = 0.4


def reference(partial_query, partial_key, partial_value, partial_mixed, partial_norm, partial_bias, master_query, master_key, master_value, master_mixed, master_norm, master_bias):
    mean_query = jnp.sum(partial_query.astype(jnp.float32), axis=0) * REPLICAS ** -0.5
    mean_key = jnp.sum(partial_key.astype(jnp.float32), axis=0) * REPLICAS ** -0.5
    mean_value = jnp.sum(partial_value.astype(jnp.float32), axis=0) * REPLICAS ** -0.5
    mean_mixed = jnp.sum(partial_mixed.astype(jnp.float32), axis=0) * REPLICAS ** -0.5
    mean_norm = jnp.sum(partial_norm.astype(jnp.float32), axis=0) * REPLICAS ** -0.5
    mean_bias = jnp.sum(partial_bias.astype(jnp.float32), axis=0) * REPLICAS ** -0.5
    stepped_query = master_query - learn_rate * mean_query
    stepped_key = master_key - learn_rate * mean_key
    stepped_value = master_value - learn_rate * mean_value
    stepped_mixed = master_mixed - learn_rate * mean_mixed
    stepped_norm = master_norm - learn_rate * mean_norm
    stepped_bias = master_bias - learn_rate * mean_bias
    compute_query = stepped_query.astype(jnp.bfloat16)
    compute_key = stepped_key.astype(jnp.bfloat16)
    compute_value = stepped_value.astype(jnp.bfloat16)
    compute_mixed = stepped_mixed.astype(jnp.bfloat16)
    compute_norm = stepped_norm.astype(jnp.bfloat16)
    compute_bias = stepped_bias.astype(jnp.bfloat16)
    return compute_query, compute_key, compute_value, compute_mixed, compute_norm, compute_bias, stepped_query, stepped_key, stepped_value, stepped_mixed, stepped_norm, stepped_bias
```

```python
import functools

import jax
import jax.numpy as jnp
from jax import lax
from jax.experimental import pallas as pl
from jax.experimental.pallas import tpu as pltpu
from jax.sharding import PartitionSpec as P

learn_rate = 0.4
HALVES = 2
SPAN = 118.0


def encode(x, limit):
    power = jnp.exp2(jnp.abs(x) * (2 * SPAN / limit) - SPAN)
    return jnp.where(x < 0, -power, power).astype(jnp.bfloat16)


def decode(code, limit):
    y = code.astype(jnp.float32)
    size = (jnp.log2(jnp.abs(y)) + SPAN) * (limit / (2 * SPAN))
    return jnp.where(y < 0, -size, size)


def kernel(n, kinds, limit, *refs):
    count = len(kinds)
    groups = n // 2
    refs = list(refs)

    def take(k):
        out = refs[:k]
        del refs[:k]
        return out

    partial, master = take(count), take(count)
    norm, bias, norm_master, bias_master = take(4)
    gathered, stepped = take(count), take(count)
    vec_all, vec_mine = take(2)
    pair_out, pair_in, part_out, part_in = take(count), take(count), take(count), take(count)
    own, vec_out, vec_in = take(count), *[take(1)[0] for _ in range(2)]
    a_send, a_recv, b_send, b_recv, c_send, c_recv, d_send, d_recv = take(8)
    v_send, v_recv, w_send, w_recv = take(4)

    rate = n ** (-0.5)
    b = lax.axis_index("batch")
    side = lax.rem(b, 2)
    g = b // 2
    partner = b + 1 - 2 * side

    def remote(src, dst, send, recv, to):
        return pltpu.make_async_remote_copy(
            src_ref=src,
            dst_ref=dst,
            send_sem=send,
            recv_sem=recv,
            device_id={"batch": to},
            device_id_type=pl.DeviceIdType.MESH,
        )

    chunks = [(a, h) for h in range(HALVES) for a in range(count)]

    def place(a, h, d):
        rows, cols = stepped[a].shape
        r = rows // HALVES
        if kinds[a] == "rows":
            return pl.ds(pl.multiple_of(d * rows + h * r, r), r), pl.ds(0, cols)
        return pl.ds(h * r, r), pl.ds(pl.multiple_of(d * cols, cols), cols)

    def load(a, h, d):
        rows, cols = place(a, h, d)
        return partial[a][0, rows, cols]

    def other(k):
        return lax.rem(g + k, groups)

    barrier = pltpu.get_barrier_semaphore()
    for k in range(1, n):
        pl.semaphore_signal(
            barrier,
            inc=1,
            device_id={"batch": lax.rem(b + k, n)},
            device_id_type=pl.DeviceIdType.MESH,
        )

    def pair_encode(c):
        a, h = chunks[c]

        def body(k, carry):
            pair_out[a][h, k] = encode(load(a, h, 2 * k + 1 - side), limit)
            return carry

        lax.fori_loop(0, groups, body, 0)

    def pair_copy(c):
        a, h = chunks[c]
        return remote(
            pair_out[a].at[h], pair_in[a].at[h], a_send.at[c], a_recv.at[c], partner
        )

    def part_copy(c, src_slot, dst_slot, to):
        a, h = chunks[c]
        return remote(
            part_out[a].at[h, src_slot],
            part_in[a].at[h, dst_slot],
            b_send.at[c, src_slot],
            b_recv.at[c, dst_slot],
            2 * to + side,
        )

    def pair_finish(c):
        a, h = chunks[c]
        pair_copy(c).wait_recv()
        for k in range(1, groups):
            to = other(k)
            total = load(a, h, 2 * to + side) + decode(pair_in[a][h, to], limit)
            part_out[a][h, to] = encode(total, 2 * limit)
            part_copy(c, to, g, to).start()
        own[a][h] = load(a, h, b) + decode(pair_in[a][h, g], limit)

    def back_copy(c, owner, slot, to):
        a, h = chunks[c]
        rows, cols = place(a, h, owner)
        block = gathered[a].at[rows, cols]
        return remote(block, block, c_send.at[c, slot], c_recv.at[c, owner // 2], to)

    def cross_copy(c, owner, recv_owner):
        a, h = chunks[c]
        rows, cols = place(a, h, owner)
        block = gathered[a].at[rows, cols]
        return remote(
            block, block, d_send.at[c, owner // 2], d_recv.at[c, recv_owner // 2], partner
        )

    def part_finish(c):
        a, h = chunks[c]
        r = stepped[a].shape[0] // HALVES
        total = own[a][h]
        for k in range(1, groups):
            source = other(k)
            part_copy(c, source, source, source).wait_recv()
            total = total + decode(part_in[a][h, source], 2 * limit)
        rows = pl.ds(h * r, r)
        new = master[a][rows, :] - learn_rate * (total * rate)
        stepped[a][rows, :] = new
        at_rows, at_cols = place(a, h, b)
        gathered[a][at_rows, at_cols] = new.astype(jnp.bfloat16)
        for k in range(1, groups):
            back_copy(c, b, k, 2 * other(k) + side).start()
        cross_copy(c, b, b).start()

    def cross_finish(c):
        for k in range(1, groups):
            owner = 2 * other(k) + side
            back_copy(c, owner, k, owner).wait_recv()
            cross_copy(c, owner, owner).start()

    def vec_copy(k):
        to = lax.rem(b + k, n)
        return remote(vec_out.at[to], vec_in.at[b], v_send.at[to], v_recv.at[b], to)

    def vec_back(k):
        to = lax.rem(b + k, n)
        return remote(vec_all.at[b], vec_all.at[b], w_send.at[to], w_recv.at[b], to)

    pair_encode(0)
    pl.semaphore_wait(barrier, n - 1)
    pair_copy(0).start()
    for d in range(n):
        vec_out[d, 0:1, :] = norm[d]
        vec_out[d, 1:2, :] = bias[d]
    for k in range(1, n):
        vec_copy(k).start()
    for c in range(1, len(chunks)):
        pair_encode(c)
        pair_copy(c).start()

    for t in range(len(chunks) + 2):
        if t < len(chunks):
            pair_finish(t)
        if 0 <= t - 1 < len(chunks):
            part_finish(t - 1)
        if t == 1:
            total = vec_out[b]
            for k in range(1, n):
                source = lax.rem(b + k, n)
                remote(
                    vec_out.at[source],
                    vec_in.at[source],
                    v_send.at[source],
                    v_recv.at[source],
                    source,
                ).wait_recv()
                total = total + vec_in[source]
            mean = total * rate
            vec_mine[0:1, :] = norm_master[...] - learn_rate * mean[0:1]
            vec_mine[1:2, :] = bias_master[...] - learn_rate * mean[1:2]
            vec_all[b] = vec_mine[...]
            for k in range(1, n):
                vec_back(k).start()
        if 0 <= t - 2 < len(chunks):
            cross_finish(t - 2)

    for c in range(len(chunks)):
        for k in range(groups):
            owner = 2 * other(k) + 1 - side
            cross_copy(c, owner, owner).wait_recv()
    for k in range(1, n):
        source = lax.rem(b + k, n)
        remote(
            vec_all.at[source],
            vec_all.at[source],
            w_send.at[source],
            w_recv.at[source],
            source,
        ).wait_recv()
    for k in range(1, n):
        vec_copy(k).wait_send()
        vec_back(k).wait_send()
    for c in range(len(chunks)):
        pair_copy(c).wait_send()
        for k in range(1, groups):
            to = other(k)
            part_copy(c, to, g, to).wait_send()
            back_copy(c, b, k, 2 * to + side).wait_send()
        for k in range(groups):
            owner = 2 * other(k) + side
            cross_copy(c, owner, owner).wait_send()


def per_device(
    partial_query,
    partial_key,
    partial_value,
    partial_mixed,
    partial_norm,
    partial_bias,
    master_query,
    master_key,
    master_value,
    master_mixed,
    master_norm,
    master_bias,
):
    n = lax.axis_size("batch")
    groups = n // 2
    limit = 0.875 if n <= 8 else 1.25
    wide = master_mixed.shape[1] % 128 == 0
    kinds = ("rows", "rows", "rows", "cols" if wide else "rows")
    if not wide:
        partial_mixed = jnp.swapaxes(partial_mixed, 1, 2)
        master_mixed = master_mixed.T
    partials = (partial_query, partial_key, partial_value, partial_mixed)
    masters = (master_query, master_key, master_value, master_mixed)
    chunk_count = len(partials) * HALVES
    w = master_norm.shape[0]

    out_shape = [jax.ShapeDtypeStruct(p.shape[1:], jnp.bfloat16) for p in partials]
    out_shape += [jax.ShapeDtypeStruct(m.shape, jnp.float32) for m in masters]
    out_shape += [
        jax.ShapeDtypeStruct((n, 2, w), jnp.float32),
        jax.ShapeDtypeStruct((2, w), jnp.float32),
    ]
    coded = [
        pltpu.VMEM((HALVES, groups, m.shape[0] // HALVES, m.shape[1]), jnp.bfloat16)
        for m in masters
    ]
    owns = [
        pltpu.VMEM((HALVES, m.shape[0] // HALVES, m.shape[1]), jnp.float32)
        for m in masters
    ]
    dma = pltpu.SemaphoreType.DMA
    vmem = pl.BlockSpec(memory_space=pltpu.VMEM)
    outs = pl.pallas_call(
        functools.partial(kernel, n, kinds, limit),
        out_shape=out_shape,
        in_specs=[vmem] * (2 * len(partials) + 4),
        out_specs=[vmem] * len(out_shape),
        scratch_shapes=coded * 4
        + owns
        + [pltpu.VMEM((n, 2, w), jnp.float32)] * 2
        + [dma((chunk_count,))] * 2
        + [dma((chunk_count, groups))] * 6
        + [dma((n,))] * 4,
        compiler_params=pltpu.CompilerParams(collective_id=0, has_side_effects=True),
    )(
        *partials,
        *masters,
        partial_norm.reshape(n, 1, w),
        partial_bias.reshape(n, 1, w),
        master_norm.reshape(1, w),
        master_bias.reshape(1, w),
    )
    computes, steppeds, (vec_all, vec_mine) = outs[:4], outs[4:8], outs[8:]
    if not wide:
        computes = (*computes[:3], computes[3].T)
        steppeds = (*steppeds[:3], steppeds[3].T)
    vec_low = vec_all.astype(jnp.bfloat16)
    return (
        *computes,
        vec_low[:, 0].reshape(-1),
        vec_low[:, 1].reshape(-1),
        *steppeds,
        vec_mine[0],
        vec_mine[1],
    )


def solution(mesh):
    in_specs = (
        P("batch", None, "cols"),
        P("batch", None, "cols"),
        P("batch", None, "cols"),
        P("batch", "cols", None),
        P("batch", None),
        P("batch", None),
        P("batch", "cols"),
        P("batch", "cols"),
        P("batch", "cols"),
        P("cols", "batch"),
        P("batch"),
        P("batch"),
    )
    out_specs = (
        P(None, "cols"),
        P(None, "cols"),
        P(None, "cols"),
        P("cols", None),
        P(),
        P(),
        P("batch", "cols"),
        P("batch", "cols"),
        P("batch", "cols"),
        P("cols", "batch"),
        P("batch"),
        P("batch"),
    )
    return jax.shard_map(
        per_device, mesh=mesh, in_specs=in_specs, out_specs=out_specs, check_vma=False
    )
```

```python
import functools

import jax
import jax.numpy as jnp
from jax import lax
from jax.experimental import pallas as pl
from jax.experimental.pallas import tpu as pltpu
from jax.sharding import PartitionSpec as P

learn_rate = 0.4
HALVES = 2
SPAN = 118.0


def encode(x, limit):
    power = jnp.exp2(jnp.abs(x) * (2 * SPAN / limit) - SPAN)
    return jnp.where(x < 0, -power, power).astype(jnp.bfloat16)


def decode(code, limit):
    y = code.astype(jnp.float32)
    size = (jnp.log2(jnp.abs(y)) + SPAN) * (limit / (2 * SPAN))
    return jnp.where(y < 0, -size, size)


def kernel(n, kinds, limit, *refs):
    count = len(kinds)
    groups = n // 2
    refs = list(refs)

    def take(k):
        out = refs[:k]
        del refs[:k]
        return out

    source, master = take(count), take(count)
    norm, bias, norm_master, bias_master = take(4)
    gathered, stepped = take(count), take(count)
    vec_all, vec_mine = take(2)
    pair_out, pair_in, part_out, part_in = take(count), take(count), take(count), take(count)
    own, partial = take(count), take(count)
    vec_out, vec_in = take(2)
    (in_sem,) = take(1)
    a_send, a_recv, b_send, b_recv, c_send, c_recv, d_send, d_recv = take(8)
    v_send, v_recv, w_send, w_recv = take(4)

    rate = n ** (-0.5)
    b = lax.axis_index("batch")
    side = lax.rem(b, 2)
    g = b // 2
    partner = b + 1 - 2 * side

    def remote(src, dst, send, recv, to):
        return pltpu.make_async_remote_copy(
            src_ref=src,
            dst_ref=dst,
            send_sem=send,
            recv_sem=recv,
            device_id={"batch": to},
            device_id_type=pl.DeviceIdType.MESH,
        )

    chunks = [(a, h) for h in range(HALVES) for a in range(count)]

    def place(a, h, d):
        rows, cols = stepped[a].shape
        r = rows // HALVES
        if kinds[a] == "rows":
            return pl.ds(pl.multiple_of(d * rows + h * r, r), r), pl.ds(0, cols)
        return pl.ds(h * r, r), pl.ds(pl.multiple_of(d * cols, cols), cols)

    def load(a, h, d):
        rows, cols = place(a, h, d)
        return partial[a][rows, cols]

    def other(k):
        return lax.rem(g + k, groups)

    loads = [
        pltpu.make_async_copy(source[a].at[0], partial[a], in_sem.at[a])
        for a in range(count)
    ]
    for copy in loads:
        copy.start()

    barrier = pltpu.get_barrier_semaphore()
    for k in range(1, n):
        pl.semaphore_signal(
            barrier,
            inc=1,
            device_id={"batch": lax.rem(b + k, n)},
            device_id_type=pl.DeviceIdType.MESH,
        )

    def pair_encode(c):
        a, h = chunks[c]

        def body(k, carry):
            pair_out[a][h, k] = encode(load(a, h, 2 * k + 1 - side), limit)
            return carry

        lax.fori_loop(0, groups, body, 0)

    def pair_copy(c):
        a, h = chunks[c]
        return remote(
            pair_out[a].at[h], pair_in[a].at[h], a_send.at[c], a_recv.at[c], partner
        )

    def part_copy(c, src_slot, dst_slot, to):
        a, h = chunks[c]
        return remote(
            part_out[a].at[h, src_slot],
            part_in[a].at[h, dst_slot],
            b_send.at[c, src_slot],
            b_recv.at[c, dst_slot],
            2 * to + side,
        )

    def pair_finish(c):
        a, h = chunks[c]
        pair_copy(c).wait_recv()
        for k in range(1, groups):
            to = other(k)
            total = load(a, h, 2 * to + side) + decode(pair_in[a][h, to], limit)
            part_out[a][h, to] = encode(total, 2 * limit)
            part_copy(c, to, g, to).start()
        own[a][h] = load(a, h, b) + decode(pair_in[a][h, g], limit)

    def line_copy(c, owner, way, to=None):
        a, h = chunks[c]
        rows, cols = place(a, h, owner)
        block = gathered[a].at[rows, cols]
        return remote(
            block,
            block,
            c_send.at[(way + 1) // 2, c, owner // 2],
            c_recv.at[c, owner // 2],
            b + 2 * way if to is None else to,
        )

    def has_next(way):
        return g < groups - 1 if way > 0 else g > 0

    def has_source(way, k):
        return g - k >= 0 if way > 0 else g + k < groups

    def cross_copy(c, owner, recv_owner):
        a, h = chunks[c]
        rows, cols = place(a, h, owner)
        block = gathered[a].at[rows, cols]
        return remote(
            block, block, d_send.at[c, owner // 2], d_recv.at[c, recv_owner // 2], partner
        )

    def part_finish(c):
        a, h = chunks[c]
        r = stepped[a].shape[0] // HALVES
        total = own[a][h]
        for k in range(1, groups):
            source = other(k)
            part_copy(c, source, source, source).wait_recv()
            total = total + decode(part_in[a][h, source], 2 * limit)
        rows = pl.ds(h * r, r)
        new = master[a][rows, :] - learn_rate * (total * rate)
        stepped[a][rows, :] = new
        at_rows, at_cols = place(a, h, b)
        gathered[a][at_rows, at_cols] = new.astype(jnp.bfloat16)
        for way in (1, -1):

            @pl.when(has_next(way))
            def _():
                line_copy(c, b, way).start()

        cross_copy(c, b, b).start()

    def line_finish(c, k):
        for way in (1, -1):

            @pl.when(has_source(way, k))
            def _():
                owner = b - 2 * k * way
                line_copy(c, owner, way, owner).wait_recv()

                @pl.when(has_next(way))
                def _():
                    line_copy(c, owner, way).start()

                cross_copy(c, owner, owner).start()

    def vec_copy(k):
        to = lax.rem(b + k, n)
        return remote(vec_out.at[to], vec_in.at[b], v_send.at[to], v_recv.at[b], to)

    def vec_back(k):
        to = lax.rem(b + k, n)
        return remote(vec_all.at[b], vec_all.at[b], w_send.at[to], w_recv.at[b], to)

    loads[0].wait()
    pair_encode(0)
    pl.semaphore_wait(barrier, n - 1)
    pair_copy(0).start()
    for d in range(n):
        vec_out[d, 0:1, :] = norm[d]
        vec_out[d, 1:2, :] = bias[d]
    for k in range(1, n):
        vec_copy(k).start()
    for c in range(1, len(chunks)):
        if c < count:
            loads[c].wait()
        pair_encode(c)
        pair_copy(c).start()

    for t in range(len(chunks) + groups):
        if t < len(chunks):
            pair_finish(t)
        if 0 <= t - 1 < len(chunks):
            part_finish(t - 1)
        if t == 1:
            total = vec_out[b]
            for k in range(1, n):
                source = lax.rem(b + k, n)
                remote(
                    vec_out.at[source],
                    vec_in.at[source],
                    v_send.at[source],
                    v_recv.at[source],
                    source,
                ).wait_recv()
                total = total + vec_in[source]
            mean = total * rate
            vec_mine[0:1, :] = norm_master[...] - learn_rate * mean[0:1]
            vec_mine[1:2, :] = bias_master[...] - learn_rate * mean[1:2]
            vec_all[b] = vec_mine[...]
            for k in range(1, n):
                vec_back(k).start()
        for k in range(groups - 1, 0, -1):
            if 0 <= t - 1 - k < len(chunks):
                line_finish(t - 1 - k, k)

    for c in range(len(chunks)):
        for k in range(groups):
            owner = 2 * other(k) + 1 - side
            cross_copy(c, owner, owner).wait_recv()
    for k in range(1, n):
        source = lax.rem(b + k, n)
        remote(
            vec_all.at[source],
            vec_all.at[source],
            w_send.at[source],
            w_recv.at[source],
            source,
        ).wait_recv()
    for k in range(1, n):
        vec_copy(k).wait_send()
        vec_back(k).wait_send()
    for c in range(len(chunks)):
        pair_copy(c).wait_send()
        for k in range(1, groups):
            to = other(k)
            part_copy(c, to, g, to).wait_send()
        for k in range(groups):
            owner = 2 * other(k) + side
            cross_copy(c, owner, owner).wait_send()
        for way in (1, -1):

            @pl.when(has_next(way))
            def _():
                line_copy(c, b, way).wait_send()

            for k in range(1, groups):

                @pl.when(has_source(way, k) & has_next(way))
                def _():
                    line_copy(c, b - 2 * k * way, way).wait_send()


def hand_over(count, *refs):
    sources, vec_all, vec_mine = refs[:count], refs[count], refs[count + 1]
    targets = refs[count + 2 : 2 * count + 2]
    norm, bias, norm_step, bias_step = refs[2 * count + 2 : 2 * count + 6]
    held = refs[2 * count + 6 : 3 * count + 6]
    in_sem, out_sem = refs[3 * count + 6 :]
    ins = [
        pltpu.make_async_copy(sources[i], held[i], in_sem.at[i]) for i in range(count)
    ]
    outs = [
        pltpu.make_async_copy(held[i], targets[i], out_sem.at[i]) for i in range(count)
    ]
    for copy in ins:
        copy.start()
    norm[...] = vec_all[:, 0, :].astype(jnp.bfloat16)
    bias[...] = vec_all[:, 1, :].astype(jnp.bfloat16)
    norm_step[...] = vec_mine[0:1, :]
    bias_step[...] = vec_mine[1:2, :]
    for i in range(count):
        ins[i].wait()
        outs[i].start()
    for copy in outs:
        copy.wait()


def per_device(
    partial_query,
    partial_key,
    partial_value,
    partial_mixed,
    partial_norm,
    partial_bias,
    master_query,
    master_key,
    master_value,
    master_mixed,
    master_norm,
    master_bias,
):
    n = lax.axis_size("batch")
    groups = n // 2
    limit = 0.875 if n <= 8 else 1.25
    wide = master_mixed.shape[1] % 128 == 0
    kinds = ("rows", "rows", "rows", "cols" if wide else "rows")
    if not wide:
        partial_mixed = jnp.swapaxes(partial_mixed, 1, 2)
        master_mixed = master_mixed.T
    partials = (partial_query, partial_key, partial_value, partial_mixed)
    masters = (master_query, master_key, master_value, master_mixed)
    chunk_count = len(partials) * HALVES
    w = master_norm.shape[0]

    out_shape = [jax.ShapeDtypeStruct(p.shape[1:], jnp.bfloat16) for p in partials]
    out_shape += [jax.ShapeDtypeStruct(m.shape, jnp.float32) for m in masters]
    out_shape += [
        jax.ShapeDtypeStruct((n, 2, w), jnp.float32),
        jax.ShapeDtypeStruct((2, w), jnp.float32),
    ]
    coded = [
        pltpu.VMEM((HALVES, groups, m.shape[0] // HALVES, m.shape[1]), jnp.bfloat16)
        for m in masters
    ]
    owns = [
        pltpu.VMEM((HALVES, m.shape[0] // HALVES, m.shape[1]), jnp.float32)
        for m in masters
    ]
    dma = pltpu.SemaphoreType.DMA
    vmem = pl.BlockSpec(memory_space=pltpu.VMEM)
    hbm = pl.BlockSpec(memory_space=pltpu.HBM)
    outs = pl.pallas_call(
        functools.partial(kernel, n, kinds, limit),
        out_shape=out_shape,
        in_specs=[hbm] * len(partials) + [vmem] * (len(partials) + 4),
        out_specs=[vmem] * len(out_shape),
        scratch_shapes=coded * 4
        + owns
        + [pltpu.VMEM(p.shape[1:], jnp.float32) for p in partials]
        + [pltpu.VMEM((n, 2, w), jnp.float32)] * 2
        + [dma((len(partials),))]
        + [dma((chunk_count,))] * 2
        + [dma((chunk_count, groups))] * 2
        + [dma((2, chunk_count, groups))]
        + [dma((chunk_count, groups))] * 3
        + [dma((n,))] * 4,
        compiler_params=pltpu.CompilerParams(collective_id=0, has_side_effects=True),
    )(
        *partials,
        *masters,
        partial_norm.reshape(n, 1, w),
        partial_bias.reshape(n, 1, w),
        master_norm.reshape(1, w),
        master_bias.reshape(1, w),
    )
    large, (vec_all, vec_mine) = outs[:8], outs[8:]
    tail_shape = [jax.ShapeDtypeStruct(x.shape, x.dtype) for x in large]
    tail_shape += [jax.ShapeDtypeStruct((n, w), jnp.bfloat16)] * 2
    tail_shape += [jax.ShapeDtypeStruct((1, w), jnp.float32)] * 2
    outs = pl.pallas_call(
        functools.partial(hand_over, len(large)),
        out_shape=tail_shape,
        in_specs=[hbm] * len(large) + [vmem] * 2,
        out_specs=[hbm] * len(large) + [vmem] * 4,
        scratch_shapes=[pltpu.VMEM(x.shape, x.dtype) for x in large]
        + [dma((len(large),))] * 2,
    )(*large, vec_all, vec_mine)
    computes, steppeds, vectors = outs[:4], outs[4:8], outs[8:]
    if not wide:
        computes = (*computes[:3], computes[3].T)
        steppeds = (*steppeds[:3], steppeds[3].T)
    norm, bias, norm_step, bias_step = (v.reshape(-1) for v in vectors)
    return (*computes, norm, bias, *steppeds, norm_step, bias_step)


def solution(mesh):
    in_specs = (
        P("batch", None, "cols"),
        P("batch", None, "cols"),
        P("batch", None, "cols"),
        P("batch", "cols", None),
        P("batch", None),
        P("batch", None),
        P("batch", "cols"),
        P("batch", "cols"),
        P("batch", "cols"),
        P("cols", "batch"),
        P("batch"),
        P("batch"),
    )
    out_specs = (
        P(None, "cols"),
        P(None, "cols"),
        P(None, "cols"),
        P("cols", None),
        P(),
        P(),
        P("batch", "cols"),
        P("batch", "cols"),
        P("batch", "cols"),
        P("cols", "batch"),
        P("batch"),
        P("batch"),
    )
    return jax.shard_map(
        per_device, mesh=mesh, in_specs=in_specs, out_specs=out_specs, check_vma=False
    )
```

```python
import functools

import jax
import jax.numpy as jnp
from jax import lax
from jax.experimental import pallas as pl
from jax.experimental.pallas import tpu as pltpu
from jax.sharding import PartitionSpec as P

learn_rate = 0.4
HALVES = 2
SPAN = 118.0


def encode(x, limit):
    power = jnp.exp2(jnp.abs(x) * (2 * SPAN / limit) - SPAN)
    return jnp.where(x < 0, -power, power).astype(jnp.bfloat16)


def decode(code, limit):
    y = code.astype(jnp.float32)
    size = (jnp.log2(jnp.abs(y)) + SPAN) * (limit / (2 * SPAN))
    return jnp.where(y < 0, -size, size)


def kernel(n, kinds, limit, *refs):
    count = len(kinds)
    groups = n // 2
    refs = list(refs)

    def take(k):
        out = refs[:k]
        del refs[:k]
        return out

    source, master = take(count), take(count)
    norm, bias, norm_master, bias_master = take(4)
    gathered, stepped = take(count), take(count)
    vec_all, vec_mine = take(2)
    pair_out, pair_in, part_out, part_in = take(count), take(count), take(count), take(count)
    own, partial = take(count), take(count)
    vec_out, vec_in = take(2)
    (in_sem,) = take(1)
    a_send, a_recv, b_send, b_recv, c_send, c_recv, d_send, d_recv = take(8)
    v_send, v_recv, w_send, w_recv = take(4)

    rate = n ** (-0.5)
    b = lax.axis_index("batch")
    side = lax.rem(b, 2)
    g = b // 2
    partner = b + 1 - 2 * side

    def remote(src, dst, send, recv, to):
        return pltpu.make_async_remote_copy(
            src_ref=src,
            dst_ref=dst,
            send_sem=send,
            recv_sem=recv,
            device_id={"batch": to},
            device_id_type=pl.DeviceIdType.MESH,
        )

    chunks = [(a, h) for h in range(HALVES) for a in range(count)]
    crossed = range(len(chunks) - len(chunks) // 4, len(chunks))

    def place(a, h, d):
        rows, cols = stepped[a].shape
        r = rows // HALVES
        if kinds[a] == "rows":
            return pl.ds(pl.multiple_of(d * rows + h * r, r), r), pl.ds(0, cols)
        return pl.ds(h * r, r), pl.ds(pl.multiple_of(d * cols, cols), cols)

    def load(a, h, d):
        rows, cols = place(a, h, d)
        return partial[a][rows, cols]

    def other(k):
        return lax.rem(g + k, groups)

    loads = [
        pltpu.make_async_copy(source[a].at[0], partial[a], in_sem.at[a])
        for a in range(count)
    ]
    for copy in loads:
        copy.start()

    barrier = pltpu.get_barrier_semaphore()
    for k in range(1, n):
        pl.semaphore_signal(
            barrier,
            inc=1,
            device_id={"batch": lax.rem(b + k, n)},
            device_id_type=pl.DeviceIdType.MESH,
        )

    def pair_encode(c):
        a, h = chunks[c]

        def body(k, carry):
            pair_out[a][h, k] = encode(load(a, h, 2 * k + 1 - side), limit)
            return carry

        lax.fori_loop(0, groups, body, 0)

    def pair_copy(c):
        a, h = chunks[c]
        return remote(
            pair_out[a].at[h], pair_in[a].at[h], a_send.at[c], a_recv.at[c], partner
        )

    def part_copy(c, src_slot, dst_slot, to):
        a, h = chunks[c]
        return remote(
            part_out[a].at[h, src_slot],
            part_in[a].at[h, dst_slot],
            b_send.at[c, src_slot],
            b_recv.at[c, dst_slot],
            2 * to + side,
        )

    def pair_finish(c):
        a, h = chunks[c]
        pair_copy(c).wait_recv()
        for k in range(1, groups):
            to = other(k)
            total = load(a, h, 2 * to + side) + decode(pair_in[a][h, to], limit)
            part_out[a][h, to] = encode(total, 2 * limit)
            part_copy(c, to, g, to).start()
        own[a][h] = load(a, h, b) + decode(pair_in[a][h, g], limit)

    def line_copy(c, owner, way, to=None):
        a, h = chunks[c]
        rows, cols = place(a, h, owner)
        block = gathered[a].at[rows, cols]
        return remote(
            block,
            block,
            c_send.at[(way + 1) // 2, c, owner],
            c_recv.at[c, owner],
            b + 2 * way if to is None else to,
        )

    def has_next(way):
        return g < groups - 1 if way > 0 else g > 0

    def has_source(way, k):
        return g - k >= 0 if way > 0 else g + k < groups

    def cross_copy(c, owner, recv_owner):
        a, h = chunks[c]
        rows, cols = place(a, h, owner)
        block = gathered[a].at[rows, cols]
        return remote(
            block, block, d_send.at[c, owner // 2], d_recv.at[c, recv_owner // 2], partner
        )

    def part_finish(c):
        a, h = chunks[c]
        r = stepped[a].shape[0] // HALVES
        total = own[a][h]
        for k in range(1, groups):
            source = other(k)
            part_copy(c, source, source, source).wait_recv()
            total = total + decode(part_in[a][h, source], 2 * limit)
        rows = pl.ds(h * r, r)
        new = master[a][rows, :] - learn_rate * (total * rate)
        stepped[a][rows, :] = new
        at_rows, at_cols = place(a, h, b)
        gathered[a][at_rows, at_cols] = new.astype(jnp.bfloat16)
        for way in (1, -1):

            @pl.when(has_next(way))
            def _():
                line_copy(c, b, way).start()

        cross_copy(c, b, b).start()

    def line_finish(c, k, shift):
        for way in (1, -1):

            @pl.when(has_source(way, k))
            def _():
                owner = b - 2 * k * way + shift
                line_copy(c, owner, way, b - 2 * k * way).wait_recv()

                @pl.when(has_next(way))
                def _():
                    line_copy(c, owner, way).start()

                if c not in crossed:
                    cross_copy(c, owner, owner).start()

    def cross_arrive(c):
        cross_copy(c, partner, partner).wait_recv()
        for way in (1, -1):

            @pl.when(has_next(way))
            def _():
                line_copy(c, partner, way).start()

    def vec_copy(k):
        to = lax.rem(b + k, n)
        return remote(vec_out.at[to], vec_in.at[b], v_send.at[to], v_recv.at[b], to)

    def vec_back(k):
        to = lax.rem(b + k, n)
        return remote(vec_all.at[b], vec_all.at[b], w_send.at[to], w_recv.at[b], to)

    loads[0].wait()
    pair_encode(0)
    pl.semaphore_wait(barrier, n - 1)
    pair_copy(0).start()
    for d in range(n):
        vec_out[d, 0:1, :] = norm[d]
        vec_out[d, 1:2, :] = bias[d]
    for k in range(1, n):
        vec_copy(k).start()
    for c in range(1, len(chunks)):
        if c < count:
            loads[c].wait()
        pair_encode(c)
        pair_copy(c).start()

    for t in range(len(chunks) + groups + 1):
        if t < len(chunks):
            pair_finish(t)
        if 0 <= t - 1 < len(chunks):
            part_finish(t - 1)
        if t == 1:
            total = vec_out[b]
            for k in range(1, n):
                source = lax.rem(b + k, n)
                remote(
                    vec_out.at[source],
                    vec_in.at[source],
                    v_send.at[source],
                    v_recv.at[source],
                    source,
                ).wait_recv()
                total = total + vec_in[source]
            mean = total * rate
            vec_mine[0:1, :] = norm_master[...] - learn_rate * mean[0:1]
            vec_mine[1:2, :] = bias_master[...] - learn_rate * mean[1:2]
            vec_all[b] = vec_mine[...]
            for k in range(1, n):
                vec_back(k).start()
        for k in range(groups - 1, 0, -1):
            if 0 <= t - 1 - k < len(chunks):
                line_finish(t - 1 - k, k, 0)
            if t - 2 - k in crossed:
                line_finish(t - 2 - k, k, partner - b)
        if t - 2 in crossed:
            cross_arrive(t - 2)

    for c in range(crossed.start):
        for k in range(groups):
            owner = 2 * other(k) + 1 - side
            cross_copy(c, owner, owner).wait_recv()
    for k in range(1, n):
        source = lax.rem(b + k, n)
        remote(
            vec_all.at[source],
            vec_all.at[source],
            w_send.at[source],
            w_recv.at[source],
            source,
        ).wait_recv()
    for k in range(1, n):
        vec_copy(k).wait_send()
        vec_back(k).wait_send()
    for c in range(len(chunks)):
        pair_copy(c).wait_send()
        for k in range(1, groups):
            to = other(k)
            part_copy(c, to, g, to).wait_send()
        for k in range(1 if c in crossed else groups):
            owner = 2 * other(k) + side
            cross_copy(c, owner, owner).wait_send()
        for shift in (0, partner - b) if c in crossed else (0,):
            for way in (1, -1):

                @pl.when(has_next(way))
                def _():
                    line_copy(c, b + shift, way).wait_send()

                for k in range(1, groups):

                    @pl.when(has_source(way, k) & has_next(way))
                    def _():
                        line_copy(c, b - 2 * k * way + shift, way).wait_send()


def hand_over(count, *refs):
    sources, vec_all, vec_mine = refs[:count], refs[count], refs[count + 1]
    targets = refs[count + 2 : 2 * count + 2]
    norm, bias, norm_step, bias_step = refs[2 * count + 2 : 2 * count + 6]
    held = refs[2 * count + 6 : 3 * count + 6]
    in_sem, out_sem = refs[3 * count + 6 :]
    ins = [
        pltpu.make_async_copy(sources[i], held[i], in_sem.at[i]) for i in range(count)
    ]
    outs = [
        pltpu.make_async_copy(held[i], targets[i], out_sem.at[i]) for i in range(count)
    ]
    for copy in ins:
        copy.start()
    norm[...] = vec_all[:, 0, :].astype(jnp.bfloat16)
    bias[...] = vec_all[:, 1, :].astype(jnp.bfloat16)
    norm_step[...] = vec_mine[0:1, :]
    bias_step[...] = vec_mine[1:2, :]
    for i in range(count):
        ins[i].wait()
        outs[i].start()
    for copy in outs:
        copy.wait()


def per_device(
    partial_query,
    partial_key,
    partial_value,
    partial_mixed,
    partial_norm,
    partial_bias,
    master_query,
    master_key,
    master_value,
    master_mixed,
    master_norm,
    master_bias,
):
    n = lax.axis_size("batch")
    groups = n // 2
    limit = 0.875 if n <= 8 else 1.25
    wide = master_mixed.shape[1] % 128 == 0
    kinds = ("rows", "rows", "rows", "cols" if wide else "rows")
    if not wide:
        partial_mixed = jnp.swapaxes(partial_mixed, 1, 2)
        master_mixed = master_mixed.T
    partials = (partial_query, partial_key, partial_value, partial_mixed)
    masters = (master_query, master_key, master_value, master_mixed)
    chunk_count = len(partials) * HALVES
    w = master_norm.shape[0]

    out_shape = [jax.ShapeDtypeStruct(p.shape[1:], jnp.bfloat16) for p in partials]
    out_shape += [jax.ShapeDtypeStruct(m.shape, jnp.float32) for m in masters]
    out_shape += [
        jax.ShapeDtypeStruct((n, 2, w), jnp.float32),
        jax.ShapeDtypeStruct((2, w), jnp.float32),
    ]
    coded = [
        pltpu.VMEM((HALVES, groups, m.shape[0] // HALVES, m.shape[1]), jnp.bfloat16)
        for m in masters
    ]
    owns = [
        pltpu.VMEM((HALVES, m.shape[0] // HALVES, m.shape[1]), jnp.float32)
        for m in masters
    ]
    dma = pltpu.SemaphoreType.DMA
    vmem = pl.BlockSpec(memory_space=pltpu.VMEM)
    hbm = pl.BlockSpec(memory_space=pltpu.HBM)
    outs = pl.pallas_call(
        functools.partial(kernel, n, kinds, limit),
        out_shape=out_shape,
        in_specs=[hbm] * len(partials) + [vmem] * (len(partials) + 4),
        out_specs=[vmem] * len(out_shape),
        scratch_shapes=coded * 4
        + owns
        + [pltpu.VMEM(p.shape[1:], jnp.float32) for p in partials]
        + [pltpu.VMEM((n, 2, w), jnp.float32)] * 2
        + [dma((len(partials),))]
        + [dma((chunk_count,))] * 2
        + [dma((chunk_count, groups))] * 2
        + [dma((2, chunk_count, n)), dma((chunk_count, n))]
        + [dma((chunk_count, groups))] * 2
        + [dma((n,))] * 4,
        compiler_params=pltpu.CompilerParams(collective_id=0, has_side_effects=True),
    )(
        *partials,
        *masters,
        partial_norm.reshape(n, 1, w),
        partial_bias.reshape(n, 1, w),
        master_norm.reshape(1, w),
        master_bias.reshape(1, w),
    )
    large, (vec_all, vec_mine) = outs[:8], outs[8:]
    tail_shape = [jax.ShapeDtypeStruct(x.shape, x.dtype) for x in large]
    tail_shape += [jax.ShapeDtypeStruct((n, w), jnp.bfloat16)] * 2
    tail_shape += [jax.ShapeDtypeStruct((1, w), jnp.float32)] * 2
    outs = pl.pallas_call(
        functools.partial(hand_over, len(large)),
        out_shape=tail_shape,
        in_specs=[hbm] * len(large) + [vmem] * 2,
        out_specs=[hbm] * len(large) + [vmem] * 4,
        scratch_shapes=[pltpu.VMEM(x.shape, x.dtype) for x in large]
        + [dma((len(large),))] * 2,
    )(*large, vec_all, vec_mine)
    computes, steppeds, vectors = outs[:4], outs[4:8], outs[8:]
    if not wide:
        computes = (*computes[:3], computes[3].T)
        steppeds = (*steppeds[:3], steppeds[3].T)
    norm, bias, norm_step, bias_step = (v.reshape(-1) for v in vectors)
    return (*computes, norm, bias, *steppeds, norm_step, bias_step)


def solution(mesh):
    in_specs = (
        P("batch", None, "cols"),
        P("batch", None, "cols"),
        P("batch", None, "cols"),
        P("batch", "cols", None),
        P("batch", None),
        P("batch", None),
        P("batch", "cols"),
        P("batch", "cols"),
        P("batch", "cols"),
        P("cols", "batch"),
        P("batch"),
        P("batch"),
    )
    out_specs = (
        P(None, "cols"),
        P(None, "cols"),
        P(None, "cols"),
        P("cols", None),
        P(),
        P(),
        P("batch", "cols"),
        P("batch", "cols"),
        P("batch", "cols"),
        P("cols", "batch"),
        P("batch"),
        P("batch"),
    )
    return jax.shard_map(
        per_device, mesh=mesh, in_specs=in_specs, out_specs=out_specs, check_vma=False
    )
```
